32 devices in a mesh: wide: 8 (over z, x), narrow: 4 (over y, core).
Axes of the slice: x: 2, y: 2, z: 4, core: 2. Of those that a mesh axis runs over, the one named last changes fastest.
Arguments:
- raw_features: bfloat16 [10240, 100], P('wide'), may hold values from -60 to 60
- placement: int32 [10240], P('wide'), may hold values from 0 to 10239, as said below
- query_counts: int32 [8], replicated, may hold values from 1 to 1024, 2048 in all
- out_grad: bfloat16 [8, 2048, 768], P('wide', 'narrow'), may hold values from -6 to 6
- w_emb: bfloat16 [100, 768], replicated, may hold values from -0.625 to 0.625
- b_emb: float32 [768], replicated, may hold values from -1.5 to 1.5
- ln1_gain: float32 [768], replicated, may hold values from 0.5 to 1.5
- ln1_bias: float32 [768], replicated, may hold values from -1.5 to 1.5
- w_qkv: bfloat16 [3, 768, 768], P(None, None, 'narrow'), may hold values from -0.21875 to 0.21875
- w_out: bfloat16 [768, 768], P('narrow'), may hold values from -3.5 to 3.5
- ln2_gain: float32 [768], replicated, may hold values from 0.5 to 1.5
- ln2_bias: float32 [768], replicated, may hold values from -1.5 to 1.5
- w_fc1: bfloat16 [768, 3072], P(None, 'narrow'), may hold values from -0.21875 to 0.21875
- b_fc1: float32 [3072], P('narrow'), may hold values from -2.5 to 2.5
- w_fc2: bfloat16 [3072, 768], P('narrow'), may hold values from -0.109375 to 0.109375
Outputs:
- layer_out: bfloat16 [8, 2048, 768], P('wide', 'narrow')
- raw_grad: float32 [10240, 100], P('wide')
- w_emb_grad: float32 [100, 768], replicated
- b_emb_grad: float32 [768], replicated
- ln1_gain_grad: float32 [768], replicated
- ln1_bias_grad: float32 [768], replicated
- w_qkv_grad: float32 [3, 768, 768], P(None, None, 'narrow')
- w_out_grad: float32 [768, 768], P('narrow')
- ln2_gain_grad: float32 [768], replicated
- ln2_bias_grad: float32 [768], replicated
- w_fc1_grad: float32 [768, 3072], P(None, 'narrow')
- b_fc1_grad: float32 [3072], P('narrow')
- w_fc2_grad: float32 [3072, 768], P('narrow')
The draws below stay inside these ranges and needn't reach their ends.
Inputs may be any that keep to these rules, and one draw needn't show every extreme that they name: `placement`: arriving row block s (rows s * 1280 to (s + 1) * 1280 - 1) holds exactly the logical rows congruent to s modulo 8, in a random order; each logical row arrives once. `query_counts`: the counts sum to 2048; the largest is exactly 1024.
All inputs are finite; a program needn't handle non-finite values.
Results may differ from the reference program's by a relative error of at most 0.0109.
Values may be sent and summed in bfloat16 or wider, within the bound.
A program may use at most 128 MiB of HBM per device.

```python
import math
import jax
import jax.numpy as jnp
import numpy as np
from jax import lax

D = 768
HEADS = 12
HD = 64
FF = 3072
FEAT = 100
CTX = 1024
QMEAN = 256
QMAX = 1024
TABLES = 8
CAP = 2048
ROWS_DEV = 1280
ROWS = 10240


def draw_raw_features(key, part):
    subkeys = jax.random.split(key, 4)
    col_scale = jnp.exp(jax.random.uniform(subkeys[0], (1, FEAT), jnp.float32, math.log(0.3), math.log(3.0)))
    col_shift = jnp.clip(jax.random.normal(subkeys[1], (1, FEAT), jnp.float32), -3.0, 3.0)
    row_scale = jnp.exp(jax.random.uniform(subkeys[2], (ROWS, 1), jnp.float32, 0.0, math.log(4.0)))
    jitter = jnp.clip(jax.random.normal(subkeys[3], (ROWS, FEAT), jnp.float32), -4.0, 4.0)
    return (col_shift + col_scale * row_scale * jitter).astype(jnp.bfloat16)


def draw_placement(key, part):
    subkeys = jax.random.split(key, TABLES)
    orders = jax.vmap(lambda one_key: jax.random.permutation(one_key, ROWS_DEV))(subkeys).astype(jnp.int32)
    return (orders * TABLES + jnp.arange(TABLES, dtype=jnp.int32)[:, None]).reshape(ROWS).astype(jnp.int32)


def block_levels(key, dims, shards, low, high):
    level = 1.0
    for position, parts in shards:
        heights = jax.random.uniform(jax.random.fold_in(jax.random.fold_in(key, 6), position), (parts,), jnp.float32, low / len(shards), high / len(shards))
        level = level * jnp.repeat(jnp.exp(heights), dims[position] // parts).reshape((-1,) + (1,) * (len(dims) - 1 - position))
    return level


def profile(number_of, total, bound, lean):
    weights = [(1 << 20) // math.isqrt(standing ** lean) + 1 for standing in range(2, number_of + 1)]
    rest, counts = total - bound - (number_of - 1), [1] * (number_of - 1)
    while rest > 0:
        movable = [i for i in range(number_of - 1) if counts[i] < bound]
        whole, budget = sum([weights[i] for i in movable]), rest
        for i in movable:
            addition = min(bound - counts[i], max(1, budget * weights[i] // whole), rest)
            counts[i] = counts[i] + addition
            rest = rest - addition
    return np.array([bound] + counts)


def uneven_parts(stream_key, number_of, total, most, lean):
    if number_of == 2:
        one = jax.random.randint(stream_key, (), max(1, total - most), min(most, total - 1) + 1)
        return jnp.stack([one, total - one])
    tallies = jnp.asarray(profile(number_of, total, most, lean), jnp.int32)
    couples = (number_of - 1) // 2
    donor, taker = tallies[1:1 + 2 * couples:2], tallies[2:2 + 2 * couples:2]
    margin = jnp.minimum(donor - 1, most - taker)
    shifted = jax.random.randint(jax.random.fold_in(stream_key, 1), (couples,), 0, 1 << 20) % (margin + 1)
    tallies = tallies.at[1:1 + 2 * couples:2].set(donor - shifted).at[2:2 + 2 * couples:2].set(taker + shifted)
    return tallies[jax.random.permutation(jax.random.fold_in(stream_key, 2), number_of)]


def gaussian(own_key, shape, deviation, bound, cuts=(), kind=jnp.bfloat16):
    entries = deviation * jax.random.normal(own_key, shape, jnp.float32)
    if cuts:
        entries = entries * block_levels(own_key, shape, cuts, -0.22, 0.18)
    return jnp.clip(entries, -bound, bound).astype(kind)


def setup_inputs(seed: int = 0) -> dict:
    key_list = jax.random.split(jax.random.key(seed), 16)
    raw_features = draw_raw_features(jax.random.fold_in(key_list[15], 71), 0)
    placement = draw_placement(jax.random.fold_in(key_list[15], 71), 0)
    query_counts = uneven_parts(key_list[2], TABLES, TABLES * QMEAN, QMAX, 2).astype(jnp.int32)
    out_grad = gaussian(key_list[3], (TABLES, CAP, D), 1.0, 6.0, ((0, 8), (1, 4)))
    w_emb = gaussian(key_list[4], (FEAT, D), FEAT ** -0.5, 0.625)
    b_emb = gaussian(key_list[5], (D,), 0.3, 1.5, (), jnp.float32)
    ln1_gain = jnp.clip(1.0 + 0.1 * jax.random.normal(key_list[6], (D,), jnp.float32), 0.5, 1.5)
    ln1_bias = gaussian(key_list[7], (D,), 0.3, 1.5, (), jnp.float32)
    w_qkv = gaussian(key_list[8], (3, D, D), D ** -0.5, 0.21875, ((2, 4),))
    w_out = gaussian(key_list[9], (D, D), (max(D // 256, 1)) ** -0.5, 3.5, ((0, 4),))
    ln2_gain = jnp.clip(1.0 + 0.1 * jax.random.normal(key_list[10], (D,), jnp.float32), 0.5, 1.5)
    ln2_bias = gaussian(key_list[11], (D,), 0.3, 1.5, (), jnp.float32)
    w_fc1 = gaussian(key_list[12], (D, FF), D ** -0.5, 0.21875, ((1, 4),))
    b_fc1 = gaussian(key_list[13], (FF,), 0.5, 2.5, ((0, 4),), jnp.float32)
    w_fc2 = gaussian(key_list[14], (FF, D), FF ** -0.5, 0.109375, ((0, 4),))
    return dict(raw_features=raw_features, placement=placement, query_counts=query_counts, out_grad=out_grad, w_emb=w_emb, b_emb=b_emb, ln1_gain=ln1_gain, ln1_bias=ln1_bias, w_qkv=w_qkv, w_out=w_out, ln2_gain=ln2_gain, ln2_bias=ln2_bias, w_fc1=w_fc1, b_fc1=b_fc1, w_fc2=w_fc2)


EPS = 1e-05
HIGHEST = lax.Precision.HIGHEST

@jax.custom_vjp
def low(v):
    return lax.optimization_barrier(v.astype(jnp.bfloat16)).astype(jnp.float32)

@jax.custom_vjp
def low_back(v):
    return v

def low_keep(v):
    return (low(v), None)

def low_pass(kept, grad):
    return (grad,)

def back_keep(v):
    return (v, None)

def back_low(kept, grad):
    return (low(grad),)
low.defvjp(low_keep, low_pass)
low_back.defvjp(back_keep, back_low)

def product(left, right):
    return jnp.dot(left, right, precision=HIGHEST)

def norm_apply(values, gain, bias):
    centre = values - lax.optimization_barrier(jnp.mean(values, -1, keepdims=True))
    spread = lax.optimization_barrier(jnp.mean(centre * centre, -1, keepdims=True))
    return centre * lax.rsqrt(spread + EPS) * gain + bias

def gelu_exact(values):
    return 0.5 * values * (1.0 + jax.scipy.special.erf(values * 0.7071067811865476))

def layer_forward(table_rows, valid_rows, params):
    w_emb, b_emb, ln1_gain, ln1_bias, w_qkv, w_out, ln2_gain, ln2_bias, w_fc1, b_fc1, w_fc2 = params
    context = table_rows[:CTX]
    row_mean = lax.optimization_barrier(jnp.sum(context, 0)) / CTX
    row_var = lax.optimization_barrier(jnp.sum(context * context, 0)) / CTX - row_mean * row_mean
    standard = low((table_rows - row_mean) * lax.rsqrt(row_var + EPS))
    embedded = low_back(product(standard, w_emb) + b_emb)
    normed_one = low(norm_apply(embedded, ln1_gain, ln1_bias))
    queries = low_back(low(product(normed_one, w_qkv[0])))
    keys_ctx = low_back(low(product(normed_one[:CTX], w_qkv[1])))
    values_ctx = low_back(low(product(normed_one[:CTX], w_qkv[2])))
    block_rows = min(512, CAP)
    score_scale = HD ** (-0.5)
    key_heads = keys_ctx.reshape(CTX, HEADS, HD)
    value_heads = values_ctx.reshape(CTX, HEADS, HD)

    def attend(query_block):
        scores = low_back(jnp.einsum('qhd,khd->hqk', query_block, key_heads, precision=HIGHEST) * score_scale)
        row_max = lax.optimization_barrier(jnp.max(scores, -1, keepdims=True))
        exp_scores = jnp.exp(scores - row_max)
        attn_probs = low(exp_scores / lax.optimization_barrier(jnp.sum(exp_scores, -1, keepdims=True)))
        return jnp.einsum('hqk,khd->qhd', attn_probs, value_heads, precision=HIGHEST).reshape(block_rows, D)
    query_heads = queries.reshape(CAP // block_rows, block_rows, HEADS, HD)
    mixed_heads = lax.map(jax.checkpoint(attend), query_heads).reshape(CAP, D)
    mixed_heads = low_back(low(mixed_heads))
    residual = embedded + low_back(product(mixed_heads, w_out))
    normed_two = low(norm_apply(residual, ln2_gain, ln2_bias))
    pre_act = low_back(product(normed_two, w_fc1) + b_fc1)
    activated = low(gelu_exact(pre_act))
    final_rows = residual + low_back(product(activated, w_fc2))
    return jnp.where(valid_rows[:, None], final_rows, 0.0)

def reference(raw_features, placement, query_counts, out_grad, w_emb, b_emb, ln1_gain, ln1_bias, w_qkv, w_out, ln2_gain, ln2_bias, w_fc1, b_fc1, w_fc2):
    starts = (jnp.arange(TABLES, dtype=jnp.int32) * CTX + jnp.cumsum(query_counts).astype(jnp.int32) - query_counts).astype(jnp.int32)
    params = tuple((value.astype(jnp.float32) for value in (w_emb, b_emb, ln1_gain, ln1_bias, w_qkv, w_out, ln2_gain, ln2_bias, w_fc1, b_fc1, w_fc2)))

    def forward(raw_values, params):
        logical = jnp.zeros((ROWS + CAP, FEAT), jnp.float32).at[placement].set(raw_values)

        def one_table(table_index):
            table_rows = lax.dynamic_slice_in_dim(logical, starts[table_index], CAP, 0)
            valid_rows = jnp.arange(CAP, dtype=jnp.int32) < CTX + query_counts[table_index]
            table_rows = jnp.where(valid_rows[:, None], table_rows, 0.0)
            return layer_forward(table_rows, valid_rows, params)
        return lax.map(jax.checkpoint(one_table), jnp.arange(TABLES, dtype=jnp.int32))
    layer_out, backward = jax.vjp(forward, raw_features.astype(jnp.float32), params)
    raw_grad, param_grads = backward(out_grad.astype(jnp.float32))
    return (layer_out.astype(jnp.bfloat16), raw_grad, param_grads[0], param_grads[1], param_grads[2], param_grads[3], param_grads[4], param_grads[5], param_grads[6], param_grads[7], param_grads[8], param_grads[9], param_grads[10])
```

```python
import functools

import jax
import jax.numpy as jnp
from jax import lax
from jax.experimental import pallas as pl
from jax.experimental.pallas import tpu as pltpu
from jax.sharding import PartitionSpec as P

HD = 64
CTX = 1024
EPS = 1e-05
LANES = 128
F32 = jnp.float32
BF16 = jnp.bfloat16
SCALE = HD ** (-0.5)


def dot(left, right):
    return jnp.dot(left, right, preferred_element_type=F32)


def dot_tn(left, right):
    return lax.dot_general(left, right, (((0,), (0,)), ((), ())), preferred_element_type=F32)


def dot_nt(left, right):
    return lax.dot_general(left, right, (((1,), (1,)), ((), ())), preferred_element_type=F32)


def full(shape):
    return pl.BlockSpec(shape, lambda *_: (0,) * len(shape))


def params():
    return pltpu.CompilerParams(dimension_semantics=("arbitrary",))


def cost(flops, moved, trans=0):
    return pl.CostEstimate(flops=int(flops), bytes_accessed=int(moved), transcendentals=int(trans))


def standardize(rows, stats_ref):
    return ((rows.astype(F32) - stats_ref[0:1, :]) * stats_ref[1:2, :]).astype(BF16)


def centre_norm(values):
    centre = values - jnp.mean(values, -1, keepdims=True)
    rstd = lax.rsqrt(jnp.mean(centre * centre, -1, keepdims=True) + EPS)
    return centre * rstd, rstd


def project_kernel(
    block, rows_ref, w_emb_ref, b_emb_ref, gain_ref, bias_ref, w_ref, q_ref, k_ref, v_ref, stats_ref
):
    step = pl.program_id(0)

    @pl.when(step == 0)
    def _():
        context = rows_ref[0:CTX, :].astype(F32)
        mean = jnp.sum(context, 0, keepdims=True) / CTX
        var = jnp.sum(context * context, 0, keepdims=True) / CTX - mean * mean
        stats_ref[...] = jnp.zeros_like(stats_ref)
        stats_ref[0:1, :] = mean
        stats_ref[1:2, :] = lax.rsqrt(var + EPS)

    start = pl.multiple_of(step * block, block)
    standard = standardize(rows_ref[pl.ds(start, block), :], stats_ref)
    embedded = dot(standard, w_emb_ref[...]) + b_emb_ref[...]
    normed = (centre_norm(embedded)[0] * gain_ref[...] + bias_ref[...]).astype(BF16)
    q_ref[...] = (dot(normed, w_ref[0]).astype(BF16) * SCALE).astype(BF16)

    @pl.when(step < CTX // block)
    def _():
        k_ref[...] = dot(normed, w_ref[1]).astype(BF16)
        v_ref[...] = dot(normed, w_ref[2]).astype(BF16)


def project(rows, w_emb, b_emb, gain, bias, w_qkv):
    capacity = rows.shape[0]
    model, width = w_emb.shape[1], w_qkv.shape[2]
    block = 256
    ctx_map = lambda b: (jnp.minimum(b, CTX // block - 1), 0)
    return pl.pallas_call(
        functools.partial(project_kernel, block),
        grid=(capacity // block,),
        in_specs=[
            full((capacity, LANES)),
            full((LANES, model)),
            full((1, model)),
            full((1, model)),
            full((1, model)),
            full((3, model, width)),
        ],
        out_specs=[
            pl.BlockSpec((block, width), lambda b: (b, 0)),
            pl.BlockSpec((block, width), ctx_map),
            pl.BlockSpec((block, width), ctx_map),
            full((8, LANES)),
        ],
        out_shape=[
            jax.ShapeDtypeStruct((capacity, width), BF16),
            jax.ShapeDtypeStruct((CTX, width), BF16),
            jax.ShapeDtypeStruct((CTX, width), BF16),
            jax.ShapeDtypeStruct((8, LANES), F32),
        ],
        compiler_params=params(),
        cost_estimate=cost(2 * capacity * model * (LANES + 2 * width), 4e6),
        name="project",
    )(rows, w_emb, b_emb, gain, bias, w_qkv)


def attend_kernel(q_ref, k_ref, v_ref, mixed_ref, log_ref):
    heads = q_ref.shape[1] // HD
    pieces = []
    for head in range(heads):
        cols = slice(head * HD, (head + 1) * HD)
        scores = dot_nt(k_ref[:, cols], q_ref[:, cols])
        top = jnp.max(scores, 0, keepdims=True)
        weights = jnp.exp(scores - top)
        total = jnp.sum(weights, 0, keepdims=True)
        probs = (weights * (1.0 / total)).astype(BF16)
        pieces.append(dot_tn(v_ref[:, cols], probs))
        log_ref[head : head + 1, :] = top + jnp.log(total)
    mixed_ref[...] = jnp.transpose(jnp.concatenate(pieces, 0)).astype(BF16)


def attend(queries, keys, values):
    capacity, width = queries.shape
    block = 256
    return pl.pallas_call(
        attend_kernel,
        grid=(capacity // block,),
        in_specs=[
            pl.BlockSpec((block, width), lambda b: (b, 0)),
            full((CTX, width)),
            full((CTX, width)),
        ],
        out_specs=[
            pl.BlockSpec((block, width), lambda b: (b, 0)),
            pl.BlockSpec((8, block), lambda b: (0, b)),
        ],
        out_shape=[
            jax.ShapeDtypeStruct((capacity, width), BF16),
            jax.ShapeDtypeStruct((8, capacity), F32),
        ],
        compiler_params=params(),
        cost_estimate=cost(8 * capacity * CTX * width, 3e6),
        name="attend",
    )(queries, keys, values)


def middle_kernel(
    count_ref,
    mixed_ref,
    rows_ref,
    stats_ref,
    w_emb_ref,
    b_emb_ref,
    gain_ref,
    bias_ref,
    out_grad_ref,
    w_out_ref,
    w_fc1_ref,
    b_fc1_ref,
    w_fc2_ref,
    layer_ref,
    mid_ref,
    mixed_grad_ref,
    g_fc1_ref,
    g_b_ref,
    g_fc2_ref,
    g_out_ref,
    g_norm_ref,
    residual_ref,
    normed_ref,
    top_ref,
    final_ref,
    back_ref,
):
    step = pl.program_id(0)
    parts, share, _ = mixed_ref.shape
    valid = lax.broadcasted_iota(jnp.int32, (share, 1), 0) < count_ref[0]

    @pl.when(step == 0)
    def _():
        standard = standardize(rows_ref[...], stats_ref)
        total = dot(standard, w_emb_ref[...]) + b_emb_ref[...]
        for part in range(parts):
            total = total + dot(mixed_ref[part], w_out_ref[part])
        residual_ref[...] = total
        normed_ref[...] = (centre_norm(total)[0] * gain_ref[...] + bias_ref[...]).astype(BF16)
        top_ref[...] = jnp.where(valid, out_grad_ref[...], jnp.zeros_like(out_grad_ref))
        final_ref[...] = jnp.zeros_like(final_ref)
        back_ref[...] = jnp.zeros_like(back_ref)

    pre = dot(normed_ref[...], w_fc1_ref[0]) + b_fc1_ref[0]
    half = 0.5 + 0.5 * lax.erf(pre * 0.7071067811865476)
    activated = (pre * half).astype(BF16)
    slope = half + pre * (0.3989422804014327 * jnp.exp(-0.5 * pre * pre))
    final_ref[...] += dot(activated, w_fc2_ref[0])
    g_fc2_ref[0] = dot_tn(activated, top_ref[...]).astype(BF16)
    pre_grad = (dot_nt(top_ref[...], w_fc2_ref[0]) * slope).astype(BF16)
    g_b_ref[0] = jnp.broadcast_to(
        jnp.sum(pre_grad.astype(F32), 0, keepdims=True), g_b_ref.shape[1:]
    )
    g_fc1_ref[0] = dot_tn(normed_ref[...], pre_grad).astype(BF16)
    back_ref[...] += dot_nt(pre_grad, w_fc1_ref[0])

    @pl.when(step == pl.num_programs(0) - 1)
    def _():
        residual = residual_ref[...]
        layer_ref[...] = jnp.where(valid, residual + final_ref[...], 0.0).astype(BF16)
        unit, rstd = centre_norm(residual)
        grad = back_ref[...]
        g_norm_ref[...] = jnp.zeros_like(g_norm_ref)
        g_norm_ref[0:1, :] = jnp.sum(grad * unit, 0, keepdims=True)
        g_norm_ref[1:2, :] = jnp.sum(grad, 0, keepdims=True)
        scaled = grad * gain_ref[...]
        mid = top_ref[...].astype(F32) + rstd * (
            scaled
            - jnp.mean(scaled, -1, keepdims=True)
            - unit * jnp.mean(scaled * unit, -1, keepdims=True)
        )
        mid_ref[...] = mid
        mid_low = mid.astype(BF16)
        for part in range(parts):
            g_out_ref[part] = dot_tn(mixed_ref[part], mid_low).astype(BF16)
            mixed_grad_ref[part] = dot_nt(mid_low, w_out_ref[part]).astype(BF16)


def middle(count, mixed, rows, stats, w_emb, b_emb, gain, bias, out_grad, w_out, w_fc1, b_fc1, w_fc2):
    parts, share, width = mixed.shape
    model, hidden = w_fc1.shape[1:]
    chunk = lambda s: (s, 0, 0)
    return pl.pallas_call(
        middle_kernel,
        grid=(parts,),
        in_specs=[
            pl.BlockSpec(memory_space=pltpu.SMEM),
            full((parts, share, width)),
            full((share, LANES)),
            full((8, LANES)),
            full((LANES, model)),
            full((1, model)),
            full((1, model)),
            full((1, model)),
            full((share, model)),
            full((parts, width, model)),
            pl.BlockSpec((1, model, hidden), chunk),
            pl.BlockSpec((1, 1, hidden), chunk),
            pl.BlockSpec((1, hidden, model), chunk),
        ],
        out_specs=[
            full((share, model)),
            full((share, model)),
            full((parts, share, width)),
            pl.BlockSpec((1, model, hidden), chunk),
            pl.BlockSpec((1, 8, hidden), chunk),
            pl.BlockSpec((1, hidden, model), chunk),
            full((parts, width, model)),
            full((8, model)),
        ],
        out_shape=[
            jax.ShapeDtypeStruct((share, model), BF16),
            jax.ShapeDtypeStruct((share, model), F32),
            jax.ShapeDtypeStruct((parts, share, width), BF16),
            jax.ShapeDtypeStruct((parts, model, hidden), BF16),
            jax.ShapeDtypeStruct((parts, 8, hidden), F32),
            jax.ShapeDtypeStruct((parts, hidden, model), BF16),
            jax.ShapeDtypeStruct((parts, width, model), BF16),
            jax.ShapeDtypeStruct((8, model), F32),
        ],
        scratch_shapes=[
            pltpu.VMEM((share, model), F32),
            pltpu.VMEM((share, model), BF16),
            pltpu.VMEM((share, model), BF16),
            pltpu.VMEM((share, model), F32),
            pltpu.VMEM((share, model), F32),
        ],
        compiler_params=params(),
        cost_estimate=cost(12 * share * model * hidden * parts * 1.3, 4e7),
        name="middle",
    )(count, mixed, rows, stats, w_emb, b_emb, gain, bias, out_grad, w_out, w_fc1, b_fc1, w_fc2)


def attend_back_kernel(
    q_ref, g_ref, log_ref, k_ref, v_ref, dq_ref, dk_ref, dv_ref, key_total, value_total
):
    step = pl.program_id(0)
    heads = q_ref.shape[1] // HD

    @pl.when(step == 0)
    def _():
        key_total[...] = jnp.zeros_like(key_total)
        value_total[...] = jnp.zeros_like(value_total)

    pieces = []
    for head in range(heads):
        cols = slice(head * HD, (head + 1) * HD)
        query, grad = q_ref[:, cols], g_ref[:, cols]
        key, value = k_ref[:, cols], v_ref[:, cols]
        probs = jnp.exp(dot_nt(key, query) - log_ref[head : head + 1, :])
        value_total[head] += dot(probs.astype(BF16), grad)
        probs_grad = dot_nt(value, grad)
        inner = jnp.sum(probs * probs_grad, 0, keepdims=True)
        score_grad = (probs * (probs_grad - inner)).astype(BF16)
        key_total[head] += dot(score_grad, query)
        pieces.append(dot_tn(key, score_grad))
    dq_ref[...] = (jnp.transpose(jnp.concatenate(pieces, 0)) * SCALE).astype(BF16)

    @pl.when(step == pl.num_programs(0) - 1)
    def _():
        for head in range(heads):
            cols = slice(head * HD, (head + 1) * HD)
            dk_ref[:, cols] = key_total[head].astype(BF16)
            dv_ref[:, cols] = value_total[head].astype(BF16)


def attend_back(queries, grads, logs, keys, values):
    capacity, width = queries.shape
    block = 256
    heads = width // HD
    return pl.pallas_call(
        attend_back_kernel,
        grid=(capacity // block,),
        in_specs=[
            pl.BlockSpec((block, width), lambda b: (b, 0)),
            pl.BlockSpec((block, width), lambda b: (b, 0)),
            pl.BlockSpec((8, block), lambda b: (0, b)),
            full((CTX, width)),
            full((CTX, width)),
        ],
        out_specs=[
            pl.BlockSpec((block, width), lambda b: (b, 0)),
            full((CTX, width)),
            full((CTX, width)),
        ],
        out_shape=[
            jax.ShapeDtypeStruct((capacity, width), BF16),
            jax.ShapeDtypeStruct((CTX, width), BF16),
            jax.ShapeDtypeStruct((CTX, width), BF16),
        ],
        scratch_shapes=[pltpu.VMEM((heads, CTX, HD), F32)] * 2,
        compiler_params=params(),
        cost_estimate=cost(20 * capacity * CTX * width, 4e6),
        name="attend_back",
    )(queries, grads, logs, keys, values)


def finish_kernel(
    block,
    place_ref,
    rows_ref,
    stats_ref,
    w_emb_ref,
    b_emb_ref,
    gain_ref,
    bias_ref,
    w_ref,
    dq_ref,
    dk_ref,
    dv_ref,
    mid_ref,
    g_w_ref,
    g_emb_ref,
    g_small_ref,
    raw_ref,
    w_total,
    back_ref,
    sums_ref,
):
    step = pl.program_id(0)
    last = pl.num_programs(0) - 1
    share = mid_ref.shape[0]
    start = pl.multiple_of(step * block, block)

    @pl.when(step == 0)
    def _():
        w_total[...] = jnp.zeros_like(w_total)
        g_emb_ref[...] = jnp.zeros_like(g_emb_ref)
        g_small_ref[...] = jnp.zeros_like(g_small_ref)
        sums_ref[...] = jnp.zeros_like(sums_ref)

    rows = rows_ref[pl.ds(start, block), :]
    standard = standardize(rows, stats_ref)
    embedded = dot(standard, w_emb_ref[...]) + b_emb_ref[...]
    unit, rstd = centre_norm(embedded)
    normed = (unit * gain_ref[...] + bias_ref[...]).astype(BF16)
    w_total[0] += dot_tn(normed, dq_ref[...])
    back_ref[...] = dot_nt(dq_ref[...], w_ref[0])

    @pl.when(step < CTX // block)
    def _():
        w_total[1] += dot_tn(normed, dk_ref[...])
        w_total[2] += dot_tn(normed, dv_ref[...])
        back_ref[...] += dot_nt(dk_ref[...], w_ref[1]) + dot_nt(dv_ref[...], w_ref[2])

    grad = back_ref[...]
    g_small_ref[0:1, :] += jnp.sum(grad * unit, 0, keepdims=True)
    g_small_ref[1:2, :] += jnp.sum(grad, 0, keepdims=True)
    scaled = grad * gain_ref[...]
    low = rstd * (
        scaled
        - jnp.mean(scaled, -1, keepdims=True)
        - unit * jnp.mean(scaled * unit, -1, keepdims=True)
    )
    back_ref[...] = low
    offset = start - place_ref[0] * share

    @pl.when((offset >= 0) & (offset < share))
    def _():
        inside = pl.multiple_of(jnp.clip(offset, 0, share - block), block)
        back_ref[...] += mid_ref[pl.ds(inside, block), :]

    low_bf = back_ref[...].astype(BF16)
    g_emb_ref[...] += dot_tn(standard, low_bf)
    g_small_ref[2:3, :] += jnp.sum(low_bf.astype(F32), 0, keepdims=True)
    standard_grad = dot_nt(low_bf, w_emb_ref[...])
    raw_ref[pl.ds(start, block), :] = standard_grad
    sums_ref[0:1, :] += jnp.sum(standard_grad, 0, keepdims=True)
    sums_ref[1:2, :] += jnp.sum(standard_grad * rows.astype(F32), 0, keepdims=True)

    @pl.when(step == last)
    def _():
        g_w_ref[...] = w_total[...].astype(BF16)
        mean, r = stats_ref[0:1, :], stats_ref[1:2, :]
        first, second = sums_ref[0:1, :], sums_ref[1:2, :]
        var_grad = -0.5 * r * r * r * (second - mean * first)
        mean_grad = -r * first - 2.0 * mean * var_grad
        context = rows_ref[0:CTX, :].astype(F32)
        raw_ref[...] = raw_ref[...] * r
        raw_ref[0:CTX, :] += (mean_grad + 2.0 * context * var_grad) / CTX


def finish(place, rows, stats, w_emb, b_emb, gain, bias, w_qkv, dq, dk, dv, mid):
    capacity = rows.shape[0]
    model, width = w_emb.shape[1], w_qkv.shape[2]
    share = mid.shape[0]
    block = 256
    ctx_map = lambda b: (jnp.minimum(b, CTX // block - 1), 0)
    return pl.pallas_call(
        functools.partial(finish_kernel, block),
        grid=(capacity // block,),
        in_specs=[
            pl.BlockSpec(memory_space=pltpu.SMEM),
            full((capacity, LANES)),
            full((8, LANES)),
            full((LANES, model)),
            full((1, model)),
            full((1, model)),
            full((1, model)),
            full((3, model, width)),
            pl.BlockSpec((block, width), lambda b: (b, 0)),
            pl.BlockSpec((block, width), ctx_map),
            pl.BlockSpec((block, width), ctx_map),
            full((share, model)),
        ],
        out_specs=[
            full((3, model, width)),
            full((LANES, model)),
            full((8, model)),
            full((capacity, LANES)),
        ],
        out_shape=[
            jax.ShapeDtypeStruct((3, model, width), BF16),
            jax.ShapeDtypeStruct((LANES, model), F32),
            jax.ShapeDtypeStruct((8, model), F32),
            jax.ShapeDtypeStruct((capacity, LANES), F32),
        ],
        scratch_shapes=[
            pltpu.VMEM((3, model, width), F32),
            pltpu.VMEM((block, model), F32),
            pltpu.VMEM((8, LANES), F32),
        ],
        compiler_params=params(),
        cost_estimate=cost(2 * capacity * model * (3 * LANES + 4 * width), 8e6),
        name="finish",
    )(place, rows, stats, w_emb, b_emb, gain, bias, w_qkv, dq, dk, dv, mid)


def shards(
    raw_features,
    placement,
    query_counts,
    out_grad,
    w_emb,
    b_emb,
    ln1_gain,
    ln1_bias,
    w_qkv,
    w_out,
    ln2_gain,
    ln2_bias,
    w_fc1,
    b_fc1,
    w_fc2,
):
    wide, parts = lax.axis_size("wide"), lax.axis_size("narrow")
    wide_index, narrow_index = lax.axis_index("wide"), lax.axis_index("narrow")
    share = out_grad.shape[1]
    capacity = share * parts
    slots = capacity // wide
    features = w_emb.shape[0]
    pad = LANES - features
    row = lambda vector: vector.reshape(1, -1)

    w_out_all = lax.all_gather(w_out, "narrow")
    w_fc1_all = lax.all_gather(w_fc1, "narrow")
    b_fc1_all = lax.all_gather(row(b_fc1), "narrow")
    w_fc2_all = lax.all_gather(w_fc2, "narrow")

    starts = (
        jnp.arange(wide, dtype=jnp.int32) * CTX + jnp.cumsum(query_counts) - query_counts
    ).astype(jnp.int32)
    table = jnp.sum((placement[:, None] >= starts[None, :]).astype(jnp.int32), 1) - 1
    member = table[:, None] == jnp.arange(wide, dtype=jnp.int32)[None, :]
    local = placement - jnp.sum(jnp.where(member, starts[None, :], 0), 1)
    slot = local // wide
    dest = table * slots + slot
    places = jnp.arange(wide * slots, dtype=jnp.int32)
    send_hot = (places[:, None] == dest[None, :]).astype(BF16)
    raw_padded = jnp.pad(raw_features, ((0, 0), (0, pad)))
    outgoing = dot(send_hot, raw_padded).astype(BF16)
    received = lax.all_to_all(outgoing.reshape(wide, slots, LANES), "wide", 0, 0, tiled=True)
    shift = jnp.remainder(starts[wide_index], wide)
    rows = jnp.transpose(jnp.roll(received, -shift, axis=0), (1, 0, 2)).reshape(capacity, LANES)

    w_emb_padded = jnp.pad(w_emb, ((0, pad), (0, 0)))
    embed = (w_emb_padded, row(b_emb))
    norm_one = (row(ln1_gain), row(ln1_bias))
    queries, keys, values, stats = project(rows, *embed, *norm_one, w_qkv)
    mixed, logs = attend(queries, keys, values)
    mixed_share = lax.all_to_all(mixed.reshape(parts, share, -1), "narrow", 0, 0, tiled=True)

    count = (CTX + query_counts[wide_index] - narrow_index * share).reshape(1)
    rows_share = lax.dynamic_slice_in_dim(rows, narrow_index * share, share, 0)
    layer_out, mid, mixed_grad, g_fc1, g_b_fc1, g_fc2, g_out, g_norm = middle(
        count,
        mixed_share,
        rows_share,
        stats,
        *embed,
        row(ln2_gain),
        row(ln2_bias),
        out_grad[0],
        w_out_all,
        w_fc1_all,
        b_fc1_all,
        w_fc2_all,
    )
    g_fc1, g_fc2, g_out, g_b_fc1 = [
        lax.psum_scatter(term, "narrow", scatter_dimension=0)
        for term in (g_fc1, g_fc2, g_out, g_b_fc1)
    ]
    grads = lax.all_to_all(mixed_grad, "narrow", 0, 0, tiled=True).reshape(capacity, -1)
    dq, dk, dv = attend_back(queries, grads, logs, keys, values)
    g_qkv, g_emb, g_small, raw_rows = finish(
        narrow_index.reshape(1), rows, stats, *embed, *norm_one, w_qkv, dq, dk, dv, mid
    )

    raw_parts = lax.all_to_all(
        raw_rows.astype(BF16).reshape(parts, share, LANES), "narrow", 0, 0, tiled=True
    )
    raw_share = jnp.sum(raw_parts.astype(F32), 0).astype(BF16)
    split = jnp.transpose(raw_share.reshape(share // wide, wide, LANES), (1, 0, 2))
    returned = lax.all_to_all(jnp.roll(split, shift, axis=0), "wide", 0, 0, tiled=True)
    gathered = lax.all_gather(returned, "narrow").reshape(-1, LANES)
    piece = slots // parts
    back = (slot // piece) * (wide * piece) + table * piece + slot % piece
    back_hot = (back[:, None] == places[None, :]).astype(BF16)
    raw_grad = dot(back_hot, gathered)[:, :features]

    small = jnp.concatenate([g_emb, g_small, g_norm], 0)
    small = lax.psum(small, ("wide", "narrow"))
    g_qkv, g_fc1, g_fc2, g_out, g_b_fc1 = lax.psum((g_qkv, g_fc1, g_fc2, g_out, g_b_fc1), "wide")
    return (
        layer_out[None],
        raw_grad,
        small[:features],
        small[LANES + 2],
        small[LANES],
        small[LANES + 1],
        g_qkv.astype(F32),
        g_out.astype(F32),
        small[LANES + 8],
        small[LANES + 9],
        g_fc1.astype(F32),
        g_b_fc1[0],
        g_fc2.astype(F32),
    )


def solution(mesh):
    in_specs = (
        P("wide", None),
        P("wide"),
        P(),
        P("wide", "narrow", None),
        P(),
        P(),
        P(),
        P(),
        P(None, None, "narrow"),
        P("narrow", None),
        P(),
        P(),
        P(None, "narrow"),
        P("narrow"),
        P("narrow", None),
    )
    out_specs = (
        P("wide", "narrow", None),
        P("wide", None),
        P(),
        P(),
        P(),
        P(),
        P(None, None, "narrow"),
        P("narrow", None),
        P(),
        P(),
        P(None, "narrow"),
        P("narrow"),
        P("narrow", None),
    )
    return jax.shard_map(shards, mesh=mesh, in_specs=in_specs, out_specs=out_specs, check_vma=False)
```
